32 devices in a mesh: gx: 4 (over x, core), gy: 2 (over y), gz: 4 (over z).
Axes of the slice: x: 2, y: 2, z: 4, core: 2. Of those that a mesh axis runs over, the one named last changes fastest.
Arguments:
- initial: float32 [64, 64, 512], P('gx', 'gy', 'gz'), may hold values from 0.5 to 2
- field_a: float32 [64, 64, 512], P('gx', 'gy', 'gz'), may hold values from -3 to 3
- field_b: float32 [64, 64, 512], P('gx', 'gy', 'gz'), may hold values from -3 to 3
- partner: float32 [3, 64, 64, 512], P(None, 'gx', 'gy', 'gz'), may hold values from 0.5 to 2
- store_a: float32 [64, 64, 512], P('gx', 'gy', 'gz'), may hold values from 0.2 to 1
- store_b: float32 [64, 64, 512], P('gx', 'gy', 'gz'), may hold values from 0.2 to 1
Outputs:
- second: float32 [64, 64, 512], P('gx', 'gy', 'gz')
- dens_a: float32 [64, 64, 512], P('gx', 'gy', 'gz')
- dens_b: float32 [64, 64, 512], P('gx', 'gy', 'gz')
- misfit: float32 [], replicated
The draws below stay inside these ranges and needn't reach their ends.
All inputs are finite; a program needn't handle non-finite values.
Results may differ from the reference program's by a relative error of at most 0.00012.
Values sent between devices are 32-bit elements; how exact they have to be, the bound alone decides.
No kernel may reach another device: no remote copies, remote signals or barrier semaphores. Data moves between devices by JAX's collectives and lax.ppermute only.
A program may use at most 64 MiB of HBM per device.

```python
import math
import jax
import jax.numpy as jnp

NX = 64
NY = 64
NZ = 512


def block_scale(own_key, dims, shards, least, largest):
    loudness, own = 1.0, jax.random.fold_in(own_key, 6)
    for axis_at, parts in shards:
        draws = jnp.exp(jax.random.uniform(jax.random.fold_in(own, axis_at), (parts,), jnp.float32, least / len(shards), largest / len(shards)))
        loudness = loudness * jnp.repeat(draws, dims[axis_at] // parts).reshape([-1 if axis == axis_at else 1 for axis in range(len(dims))])
    return loudness


def setup_inputs(seed: int = 0) -> dict:
    key_of = jax.random.split(jax.random.key(seed), 7)
    initial = jnp.clip(jnp.exp(math.log(2.0) - 1.3862944 * jax.random.uniform(key_of[0], (NX, NY, NZ), jnp.float32) ** block_scale(key_of[0], (NX, NY, NZ), ((0, 4), (1, 2), (2, 4)), -0.2, 0.2)), 0.5, 2.0)
    field_a = jnp.clip(jax.random.uniform(key_of[1], (NX, NY, NZ), jnp.float32, -3.0, 3.0) * block_scale(key_of[1], (NX, NY, NZ), ((0, 4), (1, 2), (2, 4)), -0.4, 0.0), -3.0, 3.0)
    field_b = jnp.clip(jax.random.uniform(key_of[2], (NX, NY, NZ), jnp.float32, -3.0, 3.0) * block_scale(key_of[2], (NX, NY, NZ), ((0, 4), (1, 2), (2, 4)), -0.4, 0.0), -3.0, 3.0)
    partner = jnp.clip(jnp.exp(math.log(2.0) - 1.3862944 * jax.random.uniform(key_of[3], (3, NX, NY, NZ), jnp.float32) ** block_scale(key_of[3], (3, NX, NY, NZ), ((1, 4), (2, 2), (3, 4)), -0.2, 0.2)), 0.5, 2.0)
    store_a = jnp.clip(jnp.exp(math.log(1.0) - 1.609438 * jax.random.uniform(key_of[4], (NX, NY, NZ), jnp.float32) ** block_scale(key_of[4], (NX, NY, NZ), ((0, 4), (1, 2), (2, 4)), -0.2, 0.2)), 0.2, 1.0)
    store_b = jnp.clip(jnp.exp(math.log(1.0) - 1.609438 * jax.random.uniform(key_of[5], (NX, NY, NZ), jnp.float32) ** block_scale(key_of[5], (NX, NY, NZ), ((0, 4), (1, 2), (2, 4)), -0.2, 0.2)), 0.2, 1.0)
    return {"initial": initial, "field_a": field_a, "field_b": field_b, "partner": partner, "store_a": store_a, "store_b": store_b}


contour_step = 0.25
coupling_value = 0.25 * 4096.0 / 6.0


def crank_line(values, line_dim, length):
    coupling = coupling_value
    mode_index = jnp.arange(length // 2 + 1, dtype=jnp.float32)
    eigenvalue = 2.0 * coupling * (1.0 - jnp.cos(2.0 * jnp.pi * mode_index / length))
    factor = (1.0 - eigenvalue) / (1.0 + eigenvalue)
    broadcast_shape = [1, 1, 1]
    broadcast_shape[line_dim] = length // 2 + 1
    spectrum = jnp.fft.rfft(values, axis=line_dim)
    result = jnp.fft.irfft(spectrum * factor.reshape(broadcast_shape), n=length, axis=line_dim)
    return result.astype(jnp.float32)


def advance(propagator, field):
    factor = jnp.exp(-0.5 * contour_step * field)
    values = factor * propagator
    values = crank_line(values, 0, NX)
    values = crank_line(values, 1, NY)
    values = crank_line(values, 2, NZ)
    return factor * values


def reference(initial, field_a, field_b, partner, store_a, store_b):
    first = advance(initial, field_a)
    second = advance(first, field_b)
    halfstep = 0.5 * contour_step
    raw_a = store_a + halfstep * (initial * partner[0] + first * partner[1])
    raw_b = store_b + halfstep * (first * partner[1] + second * partner[2])
    cell_total = NX * NY * NZ
    weight = jnp.sum(initial * partner[0]) / cell_total
    dens_a = raw_a / weight
    dens_b = raw_b / weight
    misfit = jnp.sum(jnp.square(dens_a + dens_b - 1.0)) / cell_total
    return second, dens_a, dens_b, misfit
```

```python
import math

import jax
import jax.numpy as jnp
from jax import lax
from jax.sharding import PartitionSpec as P

contour_step = 0.25
coupling_value = 0.25 * 4096.0 / 6.0
highest = lax.Precision.HIGHEST


def line_rate():
    small_t = 0.5 / coupling_value
    return (coupling_value, math.log(1.0 + small_t + math.sqrt(small_t * (2.0 + small_t))))


def green_scale(line_total):
    coupling, decay_rate = line_rate()
    return 1.0 / (
        2.0 * coupling * math.sinh(decay_rate) * (1.0 - math.exp(-decay_rate * line_total))
    )


def stepping_table(size_rows, line_total):
    decay_rate = line_rate()[1]
    position = jnp.arange(size_rows, dtype=jnp.float32)
    distance = jnp.abs(position[:, None] - position[None, :])
    green = green_scale(line_total) * (
        jnp.exp(-decay_rate * distance) + jnp.exp(-decay_rate * (line_total - distance))
    )
    return 2.0 * green - jnp.eye(size_rows, dtype=jnp.float32)


def along(matrix, values, line_dim):
    if line_dim == 0:
        return jnp.einsum("ij,jbc->ibc", matrix, values, precision=highest)
    if line_dim == 1:
        return jnp.einsum("ij,ajc->aic", matrix, values, precision=highest)
    return jnp.einsum("ij,abj->abi", matrix, values, precision=highest)


def block_parts(values, line_dim, line_total):
    cells = values.shape[line_dim]
    decay_rate = line_rate()[1]
    position = jnp.arange(cells, dtype=jnp.float32)
    weights = jnp.stack([jnp.exp(decay_rate * position), jnp.exp(-decay_rate * position)], axis=0)
    inside = along(stepping_table(cells, line_total), values, line_dim)
    return (inside, along(weights, values, line_dim))


def block_finish(inside, coeffs, line_dim, cells, count):
    decay_rate = line_rate()[1]
    position = jnp.arange(cells, dtype=jnp.float32)
    basis = jnp.stack([jnp.exp(-decay_rate * position), jnp.exp(decay_rate * position)], axis=1)
    return inside + 2.0 * green_scale(cells * count) * along(basis, coeffs, line_dim)


def spread_matrix(device_index, count, cells):
    decay_rate = line_rate()[1]
    blocks = jnp.arange(count, dtype=jnp.int32)
    lag_low = jnp.mod(device_index - blocks, count).astype(jnp.float32)
    lag_high = jnp.mod(blocks - device_index, count).astype(jnp.float32)
    weight_low = jnp.where(blocks == device_index, 0.0, jnp.exp(-decay_rate * cells * lag_low))
    weight_high = jnp.where(blocks == device_index, 0.0, jnp.exp(-decay_rate * cells * lag_high))
    nothing = jnp.zeros((count,), jnp.float32)
    row_plus = jnp.stack([weight_low, nothing], axis=1).reshape(2 * count)
    row_minus = jnp.stack([nothing, weight_high], axis=1).reshape(2 * count)
    return jnp.stack([row_plus, row_minus], axis=0)


def swap(values, axis, bit):
    count = lax.axis_size(axis)
    return lax.ppermute(values, axis, [(i, i ^ bit) for i in range(count)])


def bits_of(axis):
    count = lax.axis_size(axis)
    if count & (count - 1):
        raise ValueError("axis size")
    return [1 << k for k in range(count.bit_length() - 1)]


def swap_sum(value):
    for axis in ("gx", "gy", "gz"):
        for bit in bits_of(axis):
            value = value + swap(value, axis, bit)
    return value


def swap_gather(values, axis, dim):
    for bit in bits_of(axis):
        other = swap(values, axis, bit)
        upper = (lax.axis_index(axis) & bit) != 0
        values = jnp.concatenate(
            [jnp.where(upper, other, values), jnp.where(upper, values, other)], axis=dim
        )
    return values


def sweep_x(values):
    count = lax.axis_size("gx")
    cells = values.shape[0]
    inside, moments = block_parts(values, 0, cells * count)
    gathered = lax.all_gather(moments, "gx", axis=0, tiled=True)
    coeffs = along(spread_matrix(lax.axis_index("gx"), count, cells), gathered, 0)
    return block_finish(inside, coeffs, 0, cells, count)


def sweep_y(values):
    count = lax.axis_size("gy")
    cells = values.shape[1]
    inside, moments = block_parts(values, 1, cells * count)
    gathered = lax.all_gather(moments, "gy", axis=1, tiled=True)
    coeffs = along(spread_matrix(lax.axis_index("gy"), count, cells), gathered, 1)
    return block_finish(inside, coeffs, 1, cells, count)


def sweep_z(values):
    count = lax.axis_size("gz")
    cells = values.shape[2]
    inside, moments = block_parts(values, 2, cells * count)
    gathered = swap_gather(moments, "gz", 2)
    coeffs = along(spread_matrix(lax.axis_index("gz"), count, cells), gathered, 2)
    return block_finish(inside, coeffs, 2, cells, count)


def advance(propagator, field):
    factor = jnp.exp(-0.5 * contour_step * field)
    values = sweep_z(sweep_y(sweep_x(factor * propagator)))
    return factor * values


def shards(initial, field_a, field_b, partner, store_a, store_b):
    first = advance(initial, field_a)
    second = advance(first, field_b)
    halfstep = 0.5 * contour_step
    raw_a = store_a + halfstep * (initial * partner[0] + first * partner[1])
    raw_b = store_b + halfstep * (first * partner[1] + second * partner[2])
    cell_total = initial.size * lax.axis_size("gx") * lax.axis_size("gy") * lax.axis_size("gz")
    norm_sum = swap_sum(jnp.sum(initial * partner[0]))
    weight = norm_sum / cell_total
    dens_a = raw_a / weight
    dens_b = raw_b / weight
    misfit = swap_sum(jnp.sum(jnp.square(dens_a + dens_b - 1.0))) / cell_total
    return (second, dens_a, dens_b, misfit)


def solution(mesh):
    return jax.shard_map(
        shards,
        mesh=mesh,
        in_specs=(
            P("gx", "gy", "gz"),
            P("gx", "gy", "gz"),
            P("gx", "gy", "gz"),
            P(None, "gx", "gy", "gz"),
            P("gx", "gy", "gz"),
            P("gx", "gy", "gz"),
        ),
        out_specs=(P("gx", "gy", "gz"), P("gx", "gy", "gz"), P("gx", "gy", "gz"), P()),
        check_vma=False,
    )
```

```python
import functools
import math

import jax
import jax.numpy as jnp
import numpy as np
from jax import lax
from jax.experimental import pallas as pl
from jax.experimental.pallas import tpu as pltpu
from jax.sharding import PartitionSpec as P


contour_step = 0.25
halfstep = 0.5 * contour_step
coupling = 0.25 * 4096.0 / 6.0
small_t = 0.5 / coupling
decay = math.log(1.0 + small_t + math.sqrt(small_t * (2.0 + small_t)))
rho = math.exp(-decay)
gain = 1.0 / (coupling * math.sinh(decay))

AXES = ("gx", "gy", "gz")
f32 = jnp.float32
bf16 = jnp.bfloat16
TAIL = 8


def ring_table(count, cells):
    bits = count.bit_length() - 1
    table = np.zeros((count, 4 * bits + 2), np.float64)
    whole = 1.0 - math.exp(-decay * cells * count)
    for index in range(count):
        for k in range(bits):
            size = 1 << k
            place = index & (size - 1)
            step = math.exp(-decay * cells * size)
            if index & size:
                row = (math.exp(-decay * cells * place), 0.0, 1.0, step)
            else:
                row = (0.0, math.exp(-decay * cells * (size - 1 - place)), step, 1.0)
            table[index, 4 * k : 4 * k + 4] = row
        table[index, 4 * bits] = math.exp(-decay * cells * index) / whole
        table[index, 4 * bits + 1] = math.exp(-decay * cells * (count - 1 - index)) / whole
    pad = -table.shape[1] % 8
    table = np.pad(table, ((0, 0), (0, pad)))
    return np.broadcast_to(table[:, :, None], table.shape + (128,)).reshape(-1, 128).astype(np.float32)


def split(values):
    high = values.astype(jnp.bfloat16.dtype).astype(np.float64)
    return high, values - high


def line_matrix(cells):
    place = np.arange(cells, dtype=np.float64)
    inside = gain * np.exp(-decay * np.abs(place[:, None] - place[None, :])) - np.eye(cells)
    ends = np.repeat(np.exp(-decay * (cells - place))[:, None], 128, 1)
    starts = np.repeat(np.exp(-decay * place)[:, None], 128, 1)
    blocks = []
    for part in (inside, ends, starts):
        high, low = split(part)
        blocks.append(np.concatenate([high, high], 0))
        blocks.append(np.concatenate([low, np.zeros_like(low)], 0))
    return np.concatenate(blocks, 1).astype(jnp.bfloat16.dtype)


def powers(shape, dim, cells, back):
    place = lax.broadcasted_iota(jnp.int32, shape, dim).astype(f32)
    return jnp.exp(-decay * (cells - place)) if back else jnp.exp(-decay * place)


def sweep(get, put, add, count):
    front = None
    for i in range(count):
        value = get(i)
        front = value if front is None else rho * front + value
        put(i, gain * front - value)
    back = None
    for i in reversed(range(count)):
        value = get(i)
        if back is None:
            start, back = value, rho * value
        else:
            add(i, gain * back)
            start = value + back
            back = rho * start
    return rho * front, start


def moments(get, count):
    ends, starts = get(0), get(count - 1)
    for i in range(1, count):
        ends = rho * ends + get(i)
        starts = rho * starts + get(count - 1 - i)
    return rho * ends, starts


def fold(values):
    total = values[0:TAIL]
    for i in range(TAIL, values.shape[0], TAIL):
        total = total + values[i : i + TAIL]
    return total


def joined(mine, other, held, weights, bits, rows):
    k = 4 * (bits - 1)
    low, high = other[0:rows], other[rows : 2 * rows]
    before = weights[k : k + 1] * low
    after = weights[k + 1 : k + 2] * high
    if held is not None:
        before = before + held[0:rows]
        after = after + held[rows : 2 * rows]
    all_low = weights[k + 2 : k + 3] * mine[0:rows] + weights[k + 3 : k + 4] * low
    all_high = weights[k + 3 : k + 4] * mine[rows : 2 * rows] + weights[k + 2 : k + 3] * high
    before = before + weights[k + 4 : k + 5] * all_low
    after = after + weights[k + 5 : k + 6] * all_high
    return before, after


def halves(values):
    high = values.astype(bf16)
    low = (values - high.astype(f32)).astype(bf16)
    return jnp.concatenate([high, low], axis=1)


def line_step(values, matrix_ref, cells):
    both = jnp.dot(halves(values), matrix_ref[:, 0 : 2 * cells], preferred_element_type=f32)
    return both[:, 0:cells] + both[:, cells : 2 * cells]


def load_all(pairs, sems):
    copies = [pltpu.make_async_copy(source, target, sems.at[k]) for k, (source, target) in enumerate(pairs)]
    for copy in copies:
        copy.start()
    return copies


def front_kernel(a, b, init, fa, fb, part, tx, ty, tz, keep, bulk, mom, wx, wy, wz, sems):
    rows = a * b
    at = [keep.at[pl.ds(rows * k, rows)] for k in range(4)]
    copies = load_all(
        [(init, at[0]), (fa, at[1]), (fb, at[2]), (part.at[pl.ds(0, rows)], at[3])],
        sems,
    )
    for table, out, place in (
        (tx, wx, lax.axis_index("gx") // 2),
        (ty, wy, lax.axis_index("gy")),
        (tz, wz, lax.axis_index("gz")),
    ):
        size = out.shape[0] - 8
        out[0:size] = table[pl.ds(pl.multiple_of(place * size, 8), size)]
        out[size : size + 8] = jnp.full((8, 128), (lax.axis_index("gx") % 2).astype(f32))
    copies[0].wait()
    copies[1].wait()
    bulk[0:rows] = jnp.exp(-halfstep * keep[rows : 2 * rows]) * keep[0:rows]
    ends, starts = moments(lambda i: bulk[b * i : b * i + b], a)
    mom[0:b] = ends
    mom[b : 2 * b] = starts
    copies[2].wait()
    bulk[rows : 2 * rows] = jnp.exp(-halfstep * (keep[rows : 2 * rows] + keep[2 * rows : 3 * rows]))
    copies[3].wait()
    mom[2 * b : 2 * b + TAIL] = fold(keep[0:rows] * keep[3 * rows : 4 * rows])


def store_kernel(rows, keep, part, sa, sb, out, more, sems):
    at = [more.at[pl.ds(rows * k, rows)] for k in range(4)]
    copies = load_all(
        [(part.at[pl.ds(rows, rows)], at[0]), (part.at[pl.ds(2 * rows, rows)], at[1]), (sa, at[2]), (sb, at[3])],
        sems,
    )
    for copy in copies:
        copy.wait()
    init, fa, fb, p0 = (keep[rows * k : rows * k + rows] for k in range(4))
    p1, p2, la, lb = (more[rows * k : rows * k + rows] for k in range(4))
    out[0:rows] = la + lb + halfstep * (init * p0)
    out[rows : 2 * rows] = (2.0 * halfstep) * (jnp.exp(-halfstep * fa) * p1)
    out[2 * rows : 3 * rows] = halfstep * (jnp.exp(-halfstep * fb) * p2)


def is_upper(weights):
    size = weights.shape[0]
    return weights[size - 8 : size - 7] > 0.5


def pair_kernel(a, b, own, other, weights, out):
    step = math.exp(-decay * a)
    upper = is_upper(weights)
    near, far = jnp.where(upper, 1.0, step), jnp.where(upper, step, 1.0)
    out[0:b] = near * own[0:b] + far * other[0:b]
    out[b : 2 * b] = far * own[b : 2 * b] + near * other[b : 2 * b]
    out[2 * b : 2 * b + TAIL] = own[2 * b : 2 * b + TAIL] + other[2 * b : 2 * b + TAIL]


def bulk_body(get, n1, n2, lanes, matrix, z0, mom, zmom, turn, mid):
    pitch = n2 + 1

    def put(i, value):
        turn[pitch * i : pitch * i + n2] = value

    def add(i, value):
        turn[pitch * i : pitch * i + n2] += value

    sweep(get, put, add, n1)

    def put2(j, value):
        mid[n1 * j : n1 * j + n1] = value

    def add2(j, value):
        mid[n1 * j : n1 * j + n1] += value

    ends, starts = sweep(lambda j: turn[pl.ds(j, n1, stride=pitch), :], put2, add2, n2)
    mom[0:n1] = ends
    mom[n1 : 2 * n1] = starts
    lane = lax.broadcasted_iota(jnp.int32, (n1, 128), 1)
    low, high = jnp.zeros((n1, 128), f32), jnp.zeros((n1, 128), f32)
    group = 8
    for j0 in range(0, n2, group):
        here = slice(n1 * j0, n1 * (j0 + group))
        got = jnp.dot(halves(mid[here]), matrix[...], preferred_element_type=f32)
        z0[here] = got[:, 0:lanes] + got[:, lanes : 2 * lanes]
        at = 2 * lanes
        p = got[:, at : at + 128] + got[:, at + 128 : at + 256]
        q = got[:, at + 256 : at + 384] + got[:, at + 384 : at + 512]
        for j in range(group):
            low = jnp.where(lane == j0 + j, p[n1 * j : n1 * j + n1], low)
            high = jnp.where(lane == j0 + j, q[n1 * j : n1 * j + n1], high)
    zmom[0:n1] = low
    zmom[n1 : 2 * n1] = high


def bulk_first_kernel(a, b, lanes, own, other, weights, matrix, z0, mom, zmom, turned, turn, mid, both):
    n1, half = 2 * a, a * b
    pitch = b + 1
    upper = is_upper(weights)
    for k in (0, half):
        both[2 * k : 2 * k + half] = jnp.where(upper, other[k : k + half], own[k : k + half])
        both[2 * k + half : 2 * k + 2 * half] = jnp.where(upper, own[k : k + half], other[k : k + half])
    bulk_body(lambda i: both[b * i : b * i + b], n1, b, lanes, matrix, z0, mom, zmom, turn, mid)
    for i in range(n1):
        turn[pitch * i : pitch * i + b] = both[2 * half + b * i : 2 * half + b * i + b]
    for j in range(b):
        turned[n1 * j : n1 * j + n1] = turn[pl.ds(j, n1, stride=pitch), :]


def bulk_second_kernel(n1, n2, lanes, values, matrix, z0, mom, zmom, turn, mid):
    bulk_body(lambda i: values[n2 * i : n2 * i + n2], n1, n2, lanes, matrix, z0, mom, zmom, turn, mid)


def second_kernel(n1, n2, bits, mine, other, held, weights, mom, edge, out):
    low, high = joined(mine[...], other[...], None if held is None else held[...], weights[...], bits, n2)
    edge[0:n2] = low
    edge[n2 : 2 * n2] = high
    lanes = low.shape[1]
    to_end, to_start = powers((n2, lanes), 0, n2, True), powers((n2, lanes), 0, n2, False)
    up, down = gain * powers((n1, lanes), 0, n1, False), gain * powers((n1, lanes), 0, n1, True)
    for at, weight in ((0, to_end), (n1, to_start)):
        from_low = jnp.sum(weight * low, axis=0, keepdims=True)
        from_high = jnp.sum(weight * high, axis=0, keepdims=True)
        out[at : at + n1] = mom[at : at + n1] + up * from_low + down * from_high
    out[2 * n1 : 2 * n1 + TAIL] = mine[2 * n2 : 2 * n2 + TAIL] + other[2 * n2 : 2 * n2 + TAIL]


def edge_kernel(n1, n2, lanes, edge, matrix, ends, z0, zmom, value, zout, tmp):
    for at in (0, n2):
        sweep(
            lambda i: edge[at + i : at + i + 1],
            lambda i, v: tmp.__setitem__(slice(at + i, at + i + 1), v),
            lambda i, v: tmp.__setitem__(slice(at + i, at + i + 1), tmp[at + i : at + i + 1] + v),
            n2,
        )
    both = tmp[0 : 2 * n2]
    stepped = line_step(both, matrix, lanes)
    wide = jnp.concatenate([both, jnp.zeros((256 - 2 * n2, lanes), f32)], axis=0)
    rows = lax.dot_general(ends[...], wide, (((1,), (1,)), ((), ())), precision=lax.Precision.HIGHEST, preferred_element_type=f32)
    low_rows, high_rows = rows[:, 0:n2], rows[:, n2 : 2 * n2]
    up, down = gain * powers((n1, n2), 0, n1, False), gain * powers((n1, n2), 0, n1, True)
    zout[...] = zmom[...]
    for k, at in ((0, 0), (1, n1)):
        zout[at : at + n1, 0:n2] = zmom[at : at + n1, 0:n2] + up * low_rows[k : k + 1] + down * high_rows[k : k + 1]
    up, down = gain * powers((n1, lanes), 0, n1, False), gain * powers((n1, lanes), 0, n1, True)
    for j in range(n2):
        here = slice(n1 * j, n1 * j + n1)
        value[here] = z0[here] + up * stepped[j : j + 1] + down * stepped[n2 + j : n2 + j + 1]


def third_kernel(n1, n2, lanes, bits, mine, other, held, weights, zmom, edge, out):
    low, high = joined(mine[...], other[...], None if held is None else held[...], weights[...], bits, n1)
    edge[0:n1] = low
    edge[n1 : 2 * n1] = high
    up, down = gain * powers((n1, 128), 1, n2, False), gain * powers((n1, 128), 1, n2, True)
    for at, weight in ((0, powers((n1, lanes), 1, lanes, True)), (n1, powers((n1, lanes), 1, lanes, False))):
        from_low = jnp.sum(weight * low, axis=1, keepdims=True)
        from_high = jnp.sum(weight * high, axis=1, keepdims=True)
        out[at : at + n1] = zmom[at : at + n1] + up * from_low + down * from_high
    out[2 * n1 : 2 * n1 + TAIL] = mine[2 * n1 : 2 * n1 + TAIL] + other[2 * n1 : 2 * n1 + TAIL]


def fill_kernel(n1, n2, lanes, edge, matrix, value, out):
    stepped = line_step(edge[...], matrix, lanes)
    low, high = gain * stepped[0:n1], gain * stepped[n1 : 2 * n1]
    for j in range(n2):
        here = slice(n1 * j, n1 * j + n1)
        out[here] = value[here] + math.exp(-decay * j) * low + math.exp(-decay * (n2 - j)) * high


def last_terms(n1, n2, lanes, bits, mine, other, held, weights):
    low, high = joined(mine[...], other[...], None if held is None else held[...], weights[...], bits, n1)
    up, down = gain * powers((n1, lanes), 1, lanes, False), gain * powers((n1, lanes), 1, lanes, True)
    return lambda j: up * low[:, j : j + 1] + down * high[:, j : j + 1]


def middle_kernel(n1, n2, lanes, bits, mine, other, held, weights, value, factor, first, product, mom):
    term = last_terms(n1, n2, lanes, bits, mine, other, held, weights)
    for j in range(n2):
        here = slice(n1 * j, n1 * j + n1)
        got = value[here] + term(j)
        first[here] = got
        product[here] = factor[here] * got
    ends, starts = moments(lambda j: product[n1 * j : n1 * j + n1], n2)
    mom[0:n1] = ends
    mom[n1 : 2 * n1] = starts
    mom[2 * n1 : 2 * n1 + TAIL] = mine[2 * n1 : 2 * n1 + TAIL] + other[2 * n1 : 2 * n1 + TAIL]


def inverse_weight(total, cells):
    whole = jnp.sum(jnp.sum(total, axis=0, keepdims=True), axis=1, keepdims=True)
    return cells / whole


def residual_kernel(a, b, cells, first, sums, own, other, weights, back, base, slope, turn):
    n1, half = 2 * a, a * b
    pitch = n1 + 1
    inverse = inverse_weight(sums[...], cells)
    upper = is_upper(weights)
    for j in range(b):
        turn[pitch * j : pitch * j + n1] = first[n1 * j : n1 * j + n1]
    for i in range(n1):
        at = b * (i % a)
        lower_plane = i < a

        def pick(k):
            mine, theirs = own[k + at : k + at + b], other[k + at : k + at + b]
            return jnp.where(upper, theirs, mine) if lower_plane else jnp.where(upper, mine, theirs)

        value = turn[pl.ds(i, b, stride=pitch), :]
        back[b * i : b * i + b] = value
        base[b * i : b * i + b] = (pick(0) + pick(half) * value) * inverse - 1.0
        slope[b * i : b * i + b] = pick(2 * half) * inverse


def end_kernel(n1, n2, lanes, bits, mine, other, held, weights, value, base, slope, last, partial):
    term = last_terms(n1, n2, lanes, bits, mine, other, held, weights)
    total = jnp.zeros((TAIL, lanes), f32)
    for j in range(n2):
        here = slice(n1 * j, n1 * j + n1)
        got = value[here] + term(j)
        last[here] = got
        rest = base[here] + slope[here] * got
        total = total + fold(rest * rest)
    partial[...] = total


def output_kernel(rows, cells, weights, keep, more, first, last, sums, second, dens_a, dens_b):
    upper = is_upper(weights)
    one = jnp.where(upper, first[rows : 2 * rows], first[0:rows])
    two = jnp.where(upper, last[rows : 2 * rows], last[0:rows])
    inverse = inverse_weight(sums[...], cells)
    init, fa, fb, p0 = (keep[rows * k : rows * k + rows] for k in range(4))
    p1, p2, la, lb = (more[rows * k : rows * k + rows] for k in range(4))
    middle = (jnp.exp(-halfstep * fa) * one) * p1
    result = jnp.exp(-halfstep * fb) * two
    second[...] = result
    dens_a[...] = (la + halfstep * (init * p0 + middle)) * inverse
    dens_b[...] = (lb + halfstep * (middle + result * p2)) * inverse


def total_kernel(cells, mine, other, out):
    whole = mine[...] + other[...]
    whole = jnp.sum(jnp.sum(whole, axis=0, keepdims=True), axis=1, keepdims=True) * (1.0 / cells)
    out[...] = jnp.broadcast_to(whole, out.shape)


def call(kernel, name, outs, args, scratch=(), flops=100000, outside=(), sems=0):
    vmem = pl.BlockSpec(memory_space=pltpu.VMEM)
    single = not isinstance(outs, list)
    shapes = [jax.ShapeDtypeStruct(s, f32) for s in ([outs] if single else outs)]
    return pl.pallas_call(
        kernel,
        name=name,
        out_shape=shapes[0] if single else shapes,
        in_specs=[pl.BlockSpec(memory_space=pltpu.HBM) if i in outside else vmem for i in range(len(args))],
        out_specs=vmem if single else [vmem] * len(shapes),
        scratch_shapes=[pltpu.VMEM(s, f32) for s in scratch] + ([pltpu.SemaphoreType.DMA((sems,))] if sems else []),
        cost_estimate=pl.CostEstimate(flops=flops, bytes_accessed=100000, transcendentals=0),
        compiler_params=pltpu.CompilerParams(vmem_limit_bytes=16 * 1024 * 1024),
    )(*args)


def optional(kernel, held):
    if held is not None:
        return kernel
    return lambda mine, other, *rest: kernel(mine, other, None, *rest)


def some(*args):
    return [x for x in args if x is not None]


def shards(initial, field_a, field_b, partner, store_a, store_b):
    sizes = {axis: lax.axis_size(axis) for axis in AXES}
    strides = {"gx": sizes["gy"] * sizes["gz"], "gy": sizes["gz"], "gz": 1}
    devices = sizes["gx"] * sizes["gy"] * sizes["gz"]
    a, b, lanes = initial.shape
    if sizes["gx"] % 2 or any(n & (n - 1) for n in sizes.values()):
        raise ValueError("mesh size")
    n1, n2, half = 2 * a, b, a * b
    cells = float(initial.size * devices)
    counts = {"gx": sizes["gx"] // 2, "gy": sizes["gy"], "gz": sizes["gz"]}
    bits = {axis: n.bit_length() - 1 for axis, n in counts.items()}
    lengths = {"gx": n1, "gy": b, "gz": lanes}
    unit = strides["gx"]

    def pair_swap(x):
        return lax.ppermute(x, AXES, [(i, i ^ unit) for i in range(devices)])

    def swap(x, axis, k):
        mask = unit ^ ((strides[axis] << k) * (2 if axis == "gx" else 1))
        return lax.ppermute(x, AXES, [(i, i ^ mask) for i in range(devices)])

    tables = [jnp.asarray(ring_table(counts[axis], lengths[axis])) for axis in AXES]
    sized = [t.shape[0] // counts[axis] + 8 for t, axis in zip(tables, AXES)]
    matrix = jnp.asarray(line_matrix(lanes))
    place = np.arange(lanes, dtype=np.float64)
    ends = np.zeros((8, lanes), np.float32)
    ends[0], ends[1] = np.exp(-decay * (lanes - place)), np.exp(-decay * place)
    ends = jnp.asarray(ends)

    def exchange(msg, axis, rows):
        held = None
        table = weights[axis]
        for k in range(bits[axis]):
            other = swap(msg, axis, k)
            if k == bits[axis] - 1:
                return msg, other, held
            w = table[4 * k : 4 * k + 4]
            is_low = lax.broadcasted_iota(jnp.int32, (msg.shape[0], 1), 0) < rows
            is_tail = lax.broadcasted_iota(jnp.int32, (msg.shape[0], 1), 0) >= 2 * rows
            keep = jnp.where(is_low, w[0:1], jnp.where(is_tail, 0.0, w[1:2])) * other
            held = keep if held is None else held + keep
            mine = jnp.where(is_tail, 1.0, jnp.where(is_low, w[2:3], w[3:4]))
            theirs = jnp.where(is_tail, 1.0, jnp.where(is_low, w[3:4], w[2:3]))
            msg = mine * msg + theirs * other

    def step(msg, bulk, m1, m2, first, second):
        mine, other, held = exchange(msg, first, m2)
        z0, mom, zmom = bulk()
        edge, msg = call(
            optional(functools.partial(second_kernel, m1, m2, bits[first]), held),
            "second_moments",
            [(2 * m2, lanes), (2 * m1 + TAIL, lanes)],
            some(mine, other, held, weights[first], mom),
        )
        mine, other, held = exchange(msg, second, m1)
        value, zmom = call(
            functools.partial(edge_kernel, m1, m2, lanes),
            "first_edges",
            [(m1 * m2, lanes), (2 * m1, 128)],
            [edge, matrix, ends, z0, zmom],
            scratch=[(2 * m2, lanes)],
            flops=4000000,
        )
        edge, msg = call(
            optional(functools.partial(third_kernel, m1, m2, lanes, bits[second]), held),
            "third_moments",
            [(2 * m1, lanes), (2 * m1 + TAIL, 128)],
            some(mine, other, held, weights[second], zmom),
        )
        mine, other, held = exchange(msg, "gz", m1)
        value = call(
            functools.partial(fill_kernel, m1, m2, lanes),
            "second_edges",
            (m1 * m2, lanes),
            [edge, matrix, value],
            flops=4000000,
        )
        return value, mine, other, held

    flat = lambda x: x.reshape(-1, lanes)
    init, fa, fb, part = flat(initial), flat(field_a), flat(field_b), flat(partner)
    sa, sb = flat(store_a), flat(store_b)

    keep, own, msg, *tabled = call(
        functools.partial(front_kernel, a, b),
        "front",
        [(4 * half, lanes), (2 * half, lanes), (2 * b + TAIL, lanes)] + [(n, 128) for n in sized],
        [init, fa, fb, part, *tables],
        outside=(0, 1, 2, 3),
        sems=4,
    )
    weights = dict(zip(AXES, tabled))
    paired = pair_swap(msg)
    got = pair_swap(own)
    msg = call(functools.partial(pair_kernel, a, b), "pair", (2 * b + TAIL, lanes), [msg, paired, weights["gx"]])
    turned = []

    def bulk_one():
        out = call(
            functools.partial(bulk_first_kernel, a, b, lanes),
            "bulk_one",
            [(n1 * n2, lanes), (2 * n1, lanes), (2 * n1, 128), (n1 * n2, lanes)],
            [own, got, weights["gx"], matrix],
            scratch=[(n1 * (n2 + 1), lanes), (n1 * n2, lanes), (2 * n1 * n2, lanes)],
            flops=8000000,
        )
        turned.append(out[3])
        return out[0], out[1], out[2]

    stored, more = call(
        functools.partial(store_kernel, half),
        "stored",
        [(3 * half, lanes), (4 * half, lanes)],
        [keep, part, sa, sb],
        flops=4000000,
        outside=(1, 2, 3),
        sems=4,
    )
    stored_got = pair_swap(stored)
    value, mine, other, held = step(msg, bulk_one, n1, n2, "gx", "gy")
    first, product, msg = call(
        optional(functools.partial(middle_kernel, n1, n2, lanes, bits["gz"]), held),
        "middle",
        [(n1 * n2, lanes), (n1 * n2, lanes), (2 * n1 + TAIL, lanes)],
        some(mine, other, held, weights["gz"], value, turned[0]),
    )
    sums = msg[2 * n1 : 2 * n1 + TAIL]

    def bulk_two():
        return call(
            functools.partial(bulk_second_kernel, n2, n1, lanes),
            "bulk_two",
            [(n1 * n2, lanes), (2 * n2, lanes), (2 * n2, 128)],
            [product, matrix],
            scratch=[(n2 * (n1 + 1), lanes), (n1 * n2, lanes)],
            flops=8000000,
        )

    value, mine, other, held = step(msg, bulk_two, n2, n1, "gy", "gx")
    first, base, slope = call(
        functools.partial(residual_kernel, a, b, cells),
        "residual",
        [(n1 * n2, lanes)] * 3,
        [first, sums, stored, stored_got, weights["gx"]],
        scratch=[(n2 * (n1 + 1), lanes)],
        flops=4000000,
    )
    last, partial = call(
        optional(functools.partial(end_kernel, n2, n1, lanes, bits["gz"]), held),
        "end",
        [(n1 * n2, lanes), (TAIL, lanes)],
        some(mine, other, held, weights["gz"], value, base, slope),
    )
    second, dens_a, dens_b = call(
        functools.partial(output_kernel, half, cells),
        "outputs",
        [(half, lanes)] * 3,
        [weights["gx"], keep, more, first, last, sums],
        flops=4000000,
    )
    ways = [(axis, k) for axis in ("gz", "gy", "gx") for k in range(bits[axis])]
    for axis, k in ways[:-1]:
        partial = partial + swap(partial, axis, k)
    misfit = call(functools.partial(total_kernel, cells), "total", (1, 128), [partial, swap(partial, *ways[-1])])
    misfit = misfit[0, 0]
    back = lambda x: x.reshape(initial.shape)
    return back(second), back(dens_a), back(dens_b), misfit


def solution(mesh):
    grid = P("gx", "gy", "gz")
    return jax.shard_map(
        shards,
        mesh=mesh,
        in_specs=(grid, grid, grid, P(None, "gx", "gy", "gz"), grid, grid),
        out_specs=(grid, grid, grid, P()),
        check_vma=False,
    )
```

```python
import functools
import math

import jax
import jax.numpy as jnp
from jax import lax
from jax.experimental import pallas as pl
from jax.experimental.pallas import tpu as pltpu
from jax.sharding import PartitionSpec as P


contour_step = 0.25
halfstep = 0.5 * contour_step
coupling = 0.25 * 4096.0 / 6.0
small_t = 0.5 / coupling
decay = math.log(1.0 + small_t + math.sqrt(small_t * (2.0 + small_t)))
rho = math.exp(-decay)
gain = 1.0 / (coupling * math.sinh(decay))

AXES = ("gx", "gy", "gz")
f32 = jnp.float32
bf16 = jnp.bfloat16
TAIL = 8


def weight_count(count):
    return -(-(4 * (count.bit_length() - 1) + 2) // 8) * 8


def ring_weights(out, place, count, cells):
    bits = count.bit_length() - 1

    def power(steps):
        return jnp.exp(jnp.full((1, 128), steps.astype(f32) * (-decay * cells)))

    for k in range(bits):
        size = 1 << k
        inner = place & (size - 1)
        right = ((place >> k) & 1).astype(f32)
        step = math.exp(-decay * cells * size)
        out[4 * k : 4 * k + 1] = right * power(inner)
        out[4 * k + 1 : 4 * k + 2] = (1.0 - right) * power(size - 1 - inner)
        out[4 * k + 2 : 4 * k + 3] = jnp.full((1, 128), right + (1.0 - right) * step)
        out[4 * k + 3 : 4 * k + 4] = jnp.full((1, 128), right * step + (1.0 - right))
    whole = 1.0 / (1.0 - math.exp(-decay * cells * count))
    out[4 * bits : 4 * bits + 1] = whole * power(place)
    out[4 * bits + 1 : 4 * bits + 2] = whole * power(count - 1 - place)


def line_matrix(out, cells):
    shape = (cells, 128)
    far = jnp.abs(lax.broadcasted_iota(jnp.int32, shape, 0) - lax.broadcasted_iota(jnp.int32, shape, 1))
    inside = gain * jnp.exp(-decay * far.astype(f32)) - jnp.where(far == 0, 1.0, 0.0)
    ends, starts = powers(shape, 0, cells, True), powers(shape, 0, cells, False)
    parts = (inside, ends, starts, starts * starts, jnp.ones(shape, f32), ends * ends)
    for k, part in enumerate(parts):
        high = part.astype(bf16)
        at = 256 * k
        out[0:cells, at : at + 128] = high
        out[cells : 2 * cells, at : at + 128] = high
        out[0:cells, at + 128 : at + 256] = (part - high.astype(f32)).astype(bf16)
        out[cells : 2 * cells, at + 128 : at + 256] = jnp.zeros(shape, bf16)


def powers(shape, dim, cells, back):
    place = lax.broadcasted_iota(jnp.int32, shape, dim).astype(f32)
    return jnp.exp(-decay * (cells - place)) if back else jnp.exp(-decay * place)


def sweep(get, put, add, count):
    front = None
    for i in range(count):
        value = get(i)
        front = value if front is None else rho * front + value
        put(i, gain * front - value)
    back = None
    for i in reversed(range(count)):
        value = get(i)
        if back is None:
            start, back = value, rho * value
        else:
            add(i, gain * back)
            start = value + back
            back = rho * start
    return rho * front, start


def moments(get, count):
    ends, starts = get(0), get(count - 1)
    for i in range(1, count):
        ends = rho * ends + get(i)
        starts = rho * starts + get(count - 1 - i)
    return rho * ends, starts


def fold(values):
    total = values[0:TAIL]
    for i in range(TAIL, values.shape[0], TAIL):
        total = total + values[i : i + TAIL]
    return total


def joined(mine, other, held, weights, bits, rows):
    k = 4 * (bits - 1)
    low, high = other[0:rows], other[rows : 2 * rows]
    before = weights[k : k + 1] * low
    after = weights[k + 1 : k + 2] * high
    if held is not None:
        before = before + held[0:rows]
        after = after + held[rows : 2 * rows]
    all_low = weights[k + 2 : k + 3] * mine[0:rows] + weights[k + 3 : k + 4] * low
    all_high = weights[k + 3 : k + 4] * mine[rows : 2 * rows] + weights[k + 2 : k + 3] * high
    before = before + weights[k + 4 : k + 5] * all_low
    after = after + weights[k + 5 : k + 6] * all_high
    return before, after


def lane_parts(shape, width):
    lane = lax.broadcasted_iota(jnp.int32, shape, 1)
    return lane < width, (lane >= width) & (lane < 2 * width)


def packed_join(mine, other, held, weights, k, width):
    w = [weights[4 * k + i : 4 * k + i + 1] for i in range(4)]
    low, high = lane_parts(mine.shape, width)
    keep = jnp.where(low, w[0], jnp.where(high, w[1], 0.0)) * other
    if held is not None:
        keep = keep + held
    sums = jnp.where(low, w[2], w[3]) * mine + jnp.where(low, w[3], w[2]) * other
    return keep, sums


def incoming(keep, sums, weights, bits, width):
    low, _ = lane_parts(keep.shape, width)
    return keep + jnp.where(low, weights[4 * bits : 4 * bits + 1], weights[4 * bits + 1 : 4 * bits + 2]) * sums


def forms(first, second, width):
    one = [first[:, width * i : width * i + width] for i in range(4)]
    two = [second[:, width * i : width * i + width] for i in range(3)]
    return one + two


def tile_of(values):
    got = fold(values)
    if got.shape[1] == 128:
        return got
    return jnp.concatenate([got, jnp.zeros((TAIL, 128 - got.shape[1]), f32)], axis=1)


def merge_forms(mine, other, right, step):
    left = [jnp.where(right, y, x) for x, y in zip(mine, other)]
    rest = [jnp.where(right, x, y) for x, y in zip(mine, other)]
    lp, lq, l1, l2, l11, l12, l22 = left
    rp, rq, r1, r2, r11, r12, r22 = rest
    more = rq * (2.0 * l2 + l22 * rq) + lp * (2.0 * r1 + r11 * lp)
    return [
        rp + step * lp,
        lq + step * rq,
        l1 + l12 * rq + step * (r1 + r11 * lp),
        step * (l2 + l22 * rq) + r2 + r12 * lp,
        l11 + (step * step) * r11,
        step * (l12 + r12),
        (step * step) * l22 + r22,
    ], tile_of(more)


def halves(values):
    high = values.astype(bf16)
    low = (values - high.astype(f32)).astype(bf16)
    return jnp.concatenate([high, low], axis=1)


def row_sums(values, matrix_ref, at, count):
    got = jnp.dot(halves(values), matrix_ref[:, at : at + 256 * count], preferred_element_type=f32)
    return [got[:, 256 * i : 256 * i + 128] + got[:, 256 * i + 128 : 256 * i + 256] for i in range(count)]


def line_step(values, matrix_ref, cells):
    both = jnp.dot(halves(values), matrix_ref[:, 0 : 2 * cells], preferred_element_type=f32)
    return both[:, 0:cells] + both[:, cells : 2 * cells]


def front_kernel(a, b, counts, lengths, u, init, part, mom, matrix, wx, wy, wz):
    rows = a * b
    ends, starts = moments(lambda i: u[b * i : b * i + b], a)
    mom[0:b] = ends
    mom[b : 2 * b] = starts
    mom[2 * b : 2 * b + TAIL] = fold(init[...] * part[0:rows])
    places = (lax.axis_index("gx") // 2, lax.axis_index("gy"), lax.axis_index("gz"))
    for out, place, count, length in zip((wx, wy, wz), places, counts, lengths):
        ring_weights(out, place, count, length)
        size = out.shape[0] - 8
        out[size : size + 8] = jnp.full((8, 128), (lax.axis_index("gx") % 2).astype(f32))
    line_matrix(matrix, init.shape[1])


def store_kernel(rows, init, fa, fb, part, sa, sb, after, out):
    p0, p1, p2 = (part[rows * k : rows * k + rows] for k in range(3))
    first, second = jnp.exp(-halfstep * fa[...]), jnp.exp(-halfstep * fb[...])
    out[0:rows] = sa[...] + sb[...] + halfstep * (init[...] * p0)
    out[rows : 2 * rows] = (2.0 * halfstep) * (first * p1)
    out[2 * rows : 3 * rows] = halfstep * (second * p2)
    out[3 * rows : 4 * rows] = first * second


def is_upper(weights):
    size = weights.shape[0]
    return weights[size - 8 : size - 7] > 0.5


def pair_kernel(a, b, own, other, weights, out):
    step = math.exp(-decay * a)
    upper = is_upper(weights)
    near, far = jnp.where(upper, 1.0, step), jnp.where(upper, step, 1.0)
    out[0:b] = near * own[0:b] + far * other[0:b]
    out[b : 2 * b] = far * own[b : 2 * b] + near * other[b : 2 * b]
    out[2 * b : 2 * b + TAIL] = own[2 * b : 2 * b + TAIL] + other[2 * b : 2 * b + TAIL]


def bulk_body(get, n1, n2, lanes, matrix, z0, mom, zmom, turn, mid):
    pitch = n2 + 1

    def put(i, value):
        turn[pitch * i : pitch * i + n2] = value

    def add(i, value):
        turn[pitch * i : pitch * i + n2] += value

    sweep(get, put, add, n1)

    def put2(j, value):
        mid[n1 * j : n1 * j + n1] = value

    def add2(j, value):
        mid[n1 * j : n1 * j + n1] += value

    ends, starts = sweep(lambda j: turn[pl.ds(j, n1, stride=pitch), :], put2, add2, n2)
    mom[0:n1] = ends
    mom[n1 : 2 * n1] = starts
    lane = lax.broadcasted_iota(jnp.int32, (n1, 128), 1)
    packed = jnp.zeros((n1, 128), f32)
    group = 8
    for j0 in range(0, n2, group):
        here = slice(n1 * j0, n1 * (j0 + group))
        inside, p, q = row_sums(mid[here], matrix, 0, 3)
        z0[here] = inside
        for j in range(group):
            part = slice(n1 * j, n1 * j + n1)
            packed = jnp.where(lane == j0 + j, p[part], jnp.where(lane == n2 + j0 + j, q[part], packed))
    zmom[...] = packed


def bulk_first_kernel(a, b, lanes, own, other, weights, matrix, z0, mom, zmom, turn, mid, both):
    n1, half = 2 * a, a * b
    upper = is_upper(weights)
    both[0:half] = jnp.where(upper, other[...], own[...])
    both[half : 2 * half] = jnp.where(upper, own[...], other[...])
    bulk_body(lambda i: both[b * i : b * i + b], n1, b, lanes, matrix, z0, mom, zmom, turn, mid)


def factor_kernel(a, b, own, other, weights, turned, turn):
    n1, half = 2 * a, a * b
    pitch = b + 1
    upper = is_upper(weights)
    for i in range(n1):
        at = 3 * half + b * (i % a)
        mine, theirs = own[at : at + b], other[at : at + b]
        turn[pitch * i : pitch * i + b] = jnp.where(upper, theirs, mine) if i < a else jnp.where(upper, mine, theirs)
    for j in range(b):
        turned[n1 * j : n1 * j + n1] = turn[pl.ds(j, n1, stride=pitch), :]


def bulk_second_kernel(n1, n2, lanes, values, matrix, z0, mom, zmom, turn, mid):
    bulk_body(lambda i: values[n2 * i : n2 * i + n2], n1, n2, lanes, matrix, z0, mom, zmom, turn, mid)


def second_kernel(n1, n2, bits, mine, other, held, weights, mom, edge, out):
    low, high = joined(mine[...], other[...], None if held is None else held[...], weights[...], bits, n2)
    edge[0:n2] = low
    edge[n2 : 2 * n2] = high
    lanes = low.shape[1]
    to_end, to_start = powers((n2, lanes), 0, n2, True), powers((n2, lanes), 0, n2, False)
    up, down = gain * powers((n1, lanes), 0, n1, False), gain * powers((n1, lanes), 0, n1, True)
    for at, weight in ((0, to_end), (n1, to_start)):
        from_low = jnp.sum(weight * low, axis=0, keepdims=True)
        from_high = jnp.sum(weight * high, axis=0, keepdims=True)
        out[at : at + n1] = mom[at : at + n1] + up * from_low + down * from_high
    out[2 * n1 : 2 * n1 + TAIL] = mine[2 * n2 : 2 * n2 + TAIL] + other[2 * n2 : 2 * n2 + TAIL]


def edge_kernel(n1, n2, lanes, edge, matrix, z0, zmom, value, zout, tmp):
    for at in (0, n2):
        sweep(
            lambda i: edge[at + i : at + i + 1],
            lambda i, v: tmp.__setitem__(slice(at + i, at + i + 1), v),
            lambda i, v: tmp.__setitem__(slice(at + i, at + i + 1), tmp[at + i : at + i + 1] + v),
            n2,
        )
    both = tmp[0 : 2 * n2]
    stepped = row_sums(both, matrix, 0, 1)[0]
    wide = jnp.concatenate([both, jnp.zeros((256 - 2 * n2, lanes), f32)], axis=0)
    row = lax.broadcasted_iota(jnp.int32, (8, lanes), 0)
    to_end, to_start = powers((8, lanes), 1, lanes, True), powers((8, lanes), 1, lanes, False)
    ends = jnp.where(row == 0, to_end, jnp.where(row == 1, to_start, 0.0))
    rows = lax.dot_general(
        ends, wide, (((1,), (1,)), ((), ())), precision=lax.Precision.HIGHEST, preferred_element_type=f32
    )
    blank = jnp.zeros((1, 128 - 2 * n2), f32)
    low = jnp.concatenate([rows[0:1, 0:n2], rows[1:2, 0:n2], blank], axis=1)
    high = jnp.concatenate([rows[0:1, n2 : 2 * n2], rows[1:2, n2 : 2 * n2], blank], axis=1)
    up, down = gain * powers((n1, 128), 0, n1, False), gain * powers((n1, 128), 0, n1, True)
    zout[...] = zmom[...] + up * low + down * high
    for j in range(n2):
        here = slice(n1 * j, n1 * j + n1)
        value[here] = z0[here] + up * stepped[j : j + 1] + down * stepped[n2 + j : n2 + j + 1]


def third_moments(n1, n2, lanes, low, high, zmom):
    lane = lax.broadcasted_iota(jnp.int32, (n1, 128), 1)
    place = jnp.where(lane < n2, lane, lane - n2).astype(f32)
    up, down = gain * jnp.exp(-decay * place), gain * jnp.exp(-decay * (n2 - place))
    total = jnp.zeros((n1, 128), f32)
    for k, back in ((0, True), (1, False)):
        weight = powers((n1, lanes), 1, lanes, back)
        from_low = jnp.sum(weight * low, axis=1, keepdims=True)
        from_high = jnp.sum(weight * high, axis=1, keepdims=True)
        here = (lane >= n2 * k) & (lane < n2 * k + n2)
        total = jnp.where(here, up * from_low + down * from_high, total)
    return zmom + total


def third_kernel(n1, n2, lanes, bits, mine, other, held, weights, zmom, edge, out):
    low, high = joined(mine[...], other[...], None if held is None else held[...], weights[...], bits, n1)
    edge[0:n1] = low
    edge[n1 : 2 * n1] = high
    out[0:n1] = third_moments(n1, n2, lanes, low, high, zmom[...])
    out[n1 : n1 + TAIL] = mine[2 * n1 : 2 * n1 + TAIL] + other[2 * n1 : 2 * n1 + TAIL]


def third_fold_kernel(n1, n2, lanes, bits, mine, other, held, weights, zmom, value, matrix, base, slope, gram, filled, out):
    low, high = joined(mine[...], other[...], None if held is None else held[...], weights[...], bits, n1)
    moment = third_moments(n1, n2, lanes, low, high, zmom[...])
    stepped = row_sums(jnp.concatenate([low, high], axis=0), matrix, 0, 1)[0]
    low, high = gain * stepped[0:n1], gain * stepped[n1 : 2 * n1]
    lane = lax.broadcasted_iota(jnp.int32, (n1, 128), 1)
    total = jnp.zeros((TAIL, lanes), f32)
    group = 8
    for j0 in range(0, n2, group):
        products = []
        for j in range(j0, j0 + group):
            here = slice(n1 * j, n1 * j + n1)
            got = value[here] + math.exp(-decay * j) * low + math.exp(-decay * (n2 - j)) * high
            filled[here] = got
            rest = base[here] + slope[here] * got
            total = total + fold(rest * rest)
            products.append(rest * slope[here])
        p, q = row_sums(jnp.concatenate(products, axis=0), matrix, 256, 2)
        for j in range(group):
            part = slice(n1 * j, n1 * j + n1)
            at = 2 * n2 + j0 + j
            moment = jnp.where(lane == at, gain * q[part], jnp.where(lane == at + n2, gain * p[part], moment))
    out[0:n1] = moment
    out[n1 : 2 * n1] = gram[...]
    out[2 * n1 : 2 * n1 + TAIL] = total


def fill_kernel(n1, n2, lanes, edge, matrix, value, out):
    stepped = row_sums(edge[...], matrix, 0, 1)[0]
    low, high = gain * stepped[0:n1], gain * stepped[n1 : 2 * n1]
    for j in range(n2):
        here = slice(n1 * j, n1 * j + n1)
        out[here] = value[here] + math.exp(-decay * j) * low + math.exp(-decay * (n2 - j)) * high


def pack_kernel(n1, n2, k, mine, other, held, weights, keep, out):
    got, sums = packed_join(mine[0:n1], other[0:n1], None if held is None else held[...], weights[...], k, n2)
    keep[...] = got
    out[0:n1] = sums
    out[n1 : n1 + TAIL] = mine[n1 : n1 + TAIL] + other[n1 : n1 + TAIL]


def form_kernel(n1, n2, lanes, k, mine, other, held, weights, keep, out):
    w = weights[...]
    got, _ = packed_join(mine[0:n1], other[0:n1], None if held is None else held[...], w, k, n2)
    keep[...] = got
    new, tile = ring_forms(n1, n2, lanes, k, mine, other, w)
    out[0:n1] = jnp.concatenate(new[0:4] + ([] if 4 * n2 == 128 else [jnp.zeros((n1, 128 - 4 * n2), f32)]), axis=1)
    out[n1 : 2 * n1] = jnp.concatenate(new[4:7] + [jnp.zeros((n1, 128 - 3 * n2), f32)], axis=1)
    out[2 * n1 : 2 * n1 + TAIL] = tile


def ring_forms(n1, n2, lanes, k, mine, other, w):
    right = w[4 * k + 2 : 4 * k + 3, 0:n2] >= w[4 * k + 3 : 4 * k + 4, 0:n2]
    step = math.exp(-decay * lanes * (1 << k))
    own = forms(mine[0:n1], mine[n1 : 2 * n1], n2)
    theirs = forms(other[0:n1], other[n1 : 2 * n1], n2)
    new, tile = merge_forms(own, theirs, right, step)
    return new, tile + mine[2 * n1 : 2 * n1 + TAIL] + other[2 * n1 : 2 * n1 + TAIL]


def last_terms(n1, n2, lanes, bits, mine, other, held, weights):
    w = weights[...]
    keep, sums = packed_join(mine[0:n1], other[0:n1], None if held is None else held[...], w, bits - 1, n2)
    edge = incoming(keep, sums, w, bits, n2)
    up, down = gain * powers((n1, lanes), 1, lanes, False), gain * powers((n1, lanes), 1, lanes, True)
    return lambda j: up * edge[:, j : j + 1] + down * edge[:, n2 + j : n2 + j + 1]


def middle_kernel(n1, n2, lanes, bits, mine, other, held, weights, value, factor, first, product, mom):
    term = last_terms(n1, n2, lanes, bits, mine, other, held, weights)
    for j in range(n2):
        here = slice(n1 * j, n1 * j + n1)
        got = value[here] + term(j)
        first[here] = got
        product[here] = factor[here] * got
    ends, starts = moments(lambda j: product[n1 * j : n1 * j + n1], n2)
    mom[0:n1] = ends
    mom[n1 : 2 * n1] = starts
    mom[2 * n1 : 2 * n1 + TAIL] = mine[n1 : n1 + TAIL] + other[n1 : n1 + TAIL]


def inverse_weight(total, cells):
    whole = jnp.sum(jnp.sum(total, axis=0, keepdims=True), axis=1, keepdims=True)
    return cells / whole


def residual_kernel(a, b, cells, first, sums, own, other, weights, matrix, after, back, base, slope, gram, turn):
    n1, half = 2 * a, a * b
    pitch = n1 + 1
    inverse = inverse_weight(sums[...], cells)
    upper = is_upper(weights)
    lane = lax.broadcasted_iota(jnp.int32, (b, 128), 1)
    packed = jnp.zeros((b, 128), f32)
    for j in range(b):
        turn[pitch * j : pitch * j + n1] = first[n1 * j : n1 * j + n1]
    group = 8
    for i0 in range(0, n1, group):
        squares = []
        for i in range(i0, i0 + group):
            at = b * (i % a)
            lower_plane = i < a

            def pick(k):
                mine, theirs = own[k + at : k + at + b], other[k + at : k + at + b]
                return jnp.where(upper, theirs, mine) if lower_plane else jnp.where(upper, mine, theirs)

            value = turn[pl.ds(i, b, stride=pitch), :]
            back[b * i : b * i + b] = value
            base[b * i : b * i + b] = (pick(0) + pick(half) * value) * inverse - 1.0
            tilt = pick(2 * half) * inverse
            slope[b * i : b * i + b] = tilt
            squares.append(tilt * tilt)
        got = row_sums(jnp.concatenate(squares, axis=0), matrix, 768, 3)
        for k, scale in enumerate((1.0, math.exp(-decay * first.shape[1]), 1.0)):
            for i in range(group):
                here = got[k][b * i : b * i + b] * (gain * gain * scale)
                packed = jnp.where(lane == n1 * k + i0 + i, here, packed)
    gram[...] = packed


def end_kernel(n1, n2, lanes, bits, mine, other, held, weights, value, last):
    term = last_terms(n1, n2, lanes, bits, mine, other, held, weights)
    for j in range(n2):
        here = slice(n1 * j, n1 * j + n1)
        last[here] = value[here] + term(j)


def ring_kernel(n1, n2, lanes, bits, count, mine, other, weights, partial):
    new, tile = ring_forms(n1, n2, lanes, bits - 1, mine, other, weights[...])
    whole = 1.0 / (1.0 - math.exp(-decay * lanes * count))
    p, q = whole * new[0], whole * new[1]
    more = p * (2.0 * new[2] + new[4] * p) + q * (2.0 * new[3] + new[6] * q) + 2.0 * new[5] * p * q
    partial[...] = tile + tile_of(more)


def output_kernel(rows, cells, weights, init, fa, fb, part, sa, sb, first, last, sums, second, dens_a, dens_b):
    upper = is_upper(weights)
    one = jnp.where(upper, first[rows : 2 * rows], first[0:rows])
    two = jnp.where(upper, last[rows : 2 * rows], last[0:rows])
    inverse = inverse_weight(sums[...], cells)
    p0, p1, p2 = (part[rows * k : rows * k + rows] for k in range(3))
    middle = (jnp.exp(-halfstep * fa[...]) * one) * p1
    result = jnp.exp(-halfstep * fb[...]) * two
    second[...] = result
    dens_a[...] = (sa[...] + halfstep * (init[...] * p0 + middle)) * inverse
    dens_b[...] = (sb[...] + halfstep * (middle + result * p2)) * inverse


def total_kernel(cells, mine, other, out):
    whole = mine[...] + other[...]
    whole = jnp.sum(jnp.sum(whole, axis=0, keepdims=True), axis=1, keepdims=True) * (1.0 / cells)
    out[...] = jnp.broadcast_to(whole, out.shape)


def call(kernel, name, outs, args, scratch=(), flops=100000):
    vmem = pl.BlockSpec(memory_space=pltpu.VMEM)
    single = not isinstance(outs, list)
    shapes = [s if isinstance(s, jax.ShapeDtypeStruct) else jax.ShapeDtypeStruct(s, f32) for s in ([outs] if single else outs)]
    return pl.pallas_call(
        kernel,
        name=name,
        out_shape=shapes[0] if single else shapes,
        in_specs=[vmem] * len(args),
        out_specs=vmem if single else [vmem] * len(shapes),
        scratch_shapes=[pltpu.VMEM(s, f32) for s in scratch],
        cost_estimate=pl.CostEstimate(flops=flops, bytes_accessed=100000, transcendentals=0),
        compiler_params=pltpu.CompilerParams(vmem_limit_bytes=16 << 20),
    )(*args)


def optional(kernel, held):
    if held is not None:
        return kernel
    return lambda mine, other, *rest: kernel(mine, other, None, *rest)


def some(*args):
    return [x for x in args if x is not None]


def shards(initial, field_a, field_b, partner, store_a, store_b):
    sizes = {axis: lax.axis_size(axis) for axis in AXES}
    strides = {"gx": sizes["gy"] * sizes["gz"], "gy": sizes["gz"], "gz": 1}
    devices = sizes["gx"] * sizes["gy"] * sizes["gz"]
    a, b, lanes = initial.shape
    if sizes["gx"] % 2 or any(n & (n - 1) for n in sizes.values()) or lanes != 128 or 4 * max(2 * a, b) > 128:
        raise ValueError("mesh size")
    n1, n2, half = 2 * a, b, a * b
    cells = float(initial.size * devices)
    counts = {"gx": sizes["gx"] // 2, "gy": sizes["gy"], "gz": sizes["gz"]}
    bits = {axis: n.bit_length() - 1 for axis, n in counts.items()}
    lengths = {"gx": n1, "gy": b, "gz": lanes}
    unit = strides["gx"]

    def pair_swap(x):
        return lax.ppermute(x, AXES, [(i, i ^ unit) for i in range(devices)])

    def swap(x, axis, k):
        mask = unit ^ ((strides[axis] << k) * (2 if axis == "gx" else 1))
        return lax.ppermute(x, AXES, [(i, i ^ mask) for i in range(devices)])

    def exchange(msg, axis, rows):
        held = None
        table = weights[axis]
        for k in range(bits[axis]):
            other = swap(msg, axis, k)
            if k == bits[axis] - 1:
                return msg, other, held
            w = table[4 * k : 4 * k + 4]
            is_low = lax.broadcasted_iota(jnp.int32, (msg.shape[0], 1), 0) < rows
            is_tail = lax.broadcasted_iota(jnp.int32, (msg.shape[0], 1), 0) >= 2 * rows
            keep = jnp.where(is_low, w[0:1], jnp.where(is_tail, 0.0, w[1:2])) * other
            held = keep if held is None else held + keep
            mine = jnp.where(is_tail, 1.0, jnp.where(is_low, w[2:3], w[3:4]))
            theirs = jnp.where(is_tail, 1.0, jnp.where(is_low, w[3:4], w[2:3]))
            msg = mine * msg + theirs * other

    def exchange_last(msg, rows, width, fold_too):
        held = None
        for k in range(bits["gz"]):
            other = swap(msg, "gz", k)
            if k == bits["gz"] - 1:
                return msg, other, held
            kernel = functools.partial(form_kernel, rows, width, lanes, k) if fold_too else functools.partial(pack_kernel, rows, width, k)
            held, msg = call(
                optional(kernel, held),
                "between",
                [(rows, 128), msg.shape],
                some(msg, other, held, weights["gz"]),
            )

    def two_dims(msg, bulk, m1, m2, first, second):
        mine, other, held = exchange(msg, first, m2)
        z0, mom, zmom = bulk()
        edge, msg = call(
            optional(functools.partial(second_kernel, m1, m2, bits[first]), held),
            "second_moments",
            [(2 * m2, lanes), (2 * m1 + TAIL, lanes)],
            some(mine, other, held, weights[first], mom),
        )
        mine, other, held = exchange(msg, second, m1)
        value, zmom = call(
            functools.partial(edge_kernel, m1, m2, lanes),
            "first_edges",
            [(m1 * m2, lanes), (m1, 128)],
            [edge, matrix, z0, zmom],
            scratch=[(2 * m2, lanes)],
            flops=4000000,
        )
        return edge, value, zmom, mine, other, held

    flat = lambda x: x.reshape(-1, lanes)
    init, fa, fb, part = flat(initial), flat(field_a), flat(field_b), flat(partner)
    sa, sb = flat(store_a), flat(store_b)

    own = jnp.exp(-halfstep * fa) * init
    msg, matrix, *tabled = call(
        functools.partial(front_kernel, a, b, [counts[x] for x in AXES], [lengths[x] for x in AXES]),
        "front",
        [(2 * b + TAIL, lanes), jax.ShapeDtypeStruct((256, 1536), bf16)]
        + [(weight_count(counts[x]) + 8, 128) for x in AXES],
        [own, init, part],
    )
    weights = dict(zip(AXES, tabled))
    paired = pair_swap(msg)
    got = pair_swap(own)
    msg = call(functools.partial(pair_kernel, a, b), "pair", (2 * b + TAIL, lanes), [msg, paired, weights["gx"]])
    def bulk_one():
        return call(
            functools.partial(bulk_first_kernel, a, b, lanes),
            "bulk_one",
            [(n1 * n2, lanes), (2 * n1, lanes), (n1, 128)],
            [own, got, weights["gx"], matrix],
            scratch=[(n1 * (n2 + 1), lanes), (n1 * n2, lanes), (n1 * n2, lanes)],
            flops=8000000,
        )

    after, value, zmom, mine, other, held = two_dims(msg, bulk_one, n1, n2, "gx", "gy")
    edge, msg = call(
        optional(functools.partial(third_kernel, n1, n2, lanes, bits["gy"]), held),
        "third_moments",
        [(2 * n1, lanes), (n1 + TAIL, 128)],
        some(mine, other, held, weights["gy"], zmom),
    )
    mine, other, held = exchange_last(msg, n1, n2, False)
    value = call(
        functools.partial(fill_kernel, n1, n2, lanes),
        "second_edges",
        (n1 * n2, lanes),
        [edge, matrix, value],
        flops=4000000,
    )
    stored = call(
        functools.partial(store_kernel, half),
        "stored",
        (4 * half, lanes),
        [init, fa, fb, part, sa, sb, after],
        flops=4000000,
    )
    stored_got = pair_swap(stored)
    turned = call(
        functools.partial(factor_kernel, a, b),
        "turned",
        (n1 * n2, lanes),
        [stored, stored_got, weights["gx"]],
        scratch=[(n1 * (n2 + 1), lanes)],
        flops=4000000,
    )
    first, product, msg = call(
        optional(functools.partial(middle_kernel, n1, n2, lanes, bits["gz"]), held),
        "middle",
        [(n1 * n2, lanes), (n1 * n2, lanes), (2 * n1 + TAIL, lanes)],
        some(mine, other, held, weights["gz"], value, turned),
    )
    sums = msg[2 * n1 : 2 * n1 + TAIL]

    def bulk_two():
        return call(
            functools.partial(bulk_second_kernel, n2, n1, lanes),
            "bulk_two",
            [(n1 * n2, lanes), (2 * n2, lanes), (n2, 128)],
            [product, matrix],
            scratch=[(n2 * (n1 + 1), lanes), (n1 * n2, lanes)],
            flops=8000000,
        )

    edge, value, zmom, mine, other, held = two_dims(msg, bulk_two, n2, n1, "gy", "gx")
    first, base, slope, gram = call(
        functools.partial(residual_kernel, a, b, cells),
        "residual",
        [(n1 * n2, lanes)] * 3 + [(n2, 128)],
        [first, sums, stored, stored_got, weights["gx"], matrix, edge],
        scratch=[(n2 * (n1 + 1), lanes)],
        flops=4000000,
    )
    value, msg = call(
        optional(functools.partial(third_fold_kernel, n2, n1, lanes, bits["gx"]), held),
        "third_moments",
        [(n1 * n2, lanes), (2 * n2 + TAIL, 128)],
        some(mine, other, held, weights["gx"], zmom, value, matrix, base, slope, gram),
    )
    mine, other, held = exchange_last(msg, n2, n1, True)
    partial = call(
        functools.partial(ring_kernel, n2, n1, lanes, bits["gz"], counts["gz"]),
        "ring",
        (TAIL, 128),
        [mine, other, weights["gz"]],
    )
    last = call(
        optional(functools.partial(end_kernel, n2, n1, lanes, bits["gz"]), held),
        "end",
        (n1 * n2, lanes),
        some(mine, other, held, weights["gz"], value),
        flops=4000000,
    )
    second, dens_a, dens_b = call(
        functools.partial(output_kernel, half, cells),
        "outputs",
        [(half, lanes)] * 3,
        [weights["gx"], init, fa, fb, part, sa, sb, first, last, sums],
        flops=4000000,
    )
    ways = [(axis, k) for axis in ("gy", "gx") for k in range(bits[axis])]
    for axis, k in ways[:-1]:
        partial = partial + swap(partial, axis, k)
    misfit = call(functools.partial(total_kernel, cells), "total", (1, 128), [partial, swap(partial, *ways[-1])])
    misfit = misfit[0, 0]
    back = lambda x: x.reshape(initial.shape)
    return back(second), back(dens_a), back(dens_b), misfit


def solution(mesh):
    grid = P("gx", "gy", "gz")
    return jax.shard_map(
        shards,
        mesh=mesh,
        in_specs=(grid, grid, grid, P(None, "gx", "gy", "gz"), grid, grid),
        out_specs=(grid, grid, grid, P()),
        check_vma=False,
    )
```
